32 devices in a mesh: pb: 2 (over x), col: 16 (over z, y, core).
Axes of the slice: x: 2, y: 2, z: 4, core: 2. Of those that a mesh axis runs over, the one named last changes fastest.
Arguments:
- queries: bfloat16 [4096, 1024], P(('pb', 'col')), may hold values from -64 to 64
- candidates: bfloat16 [16384, 1024], P(('col', 'pb')), may hold values from -5 to 5
- grades: int32 [4096, 16384], P('pb', 'col'), may hold values from 0 to 4
- query_weights: float32 [4096], P('pb'), may hold values from -0.046875 to 0.046875
Outputs:
- losses: float32 [4096], P('pb')
- query_grad: bfloat16 [4096, 1024], P(('pb', 'col'))
- cand_grad: bfloat16 [16384, 1024], P(('col', 'pb'))
The draws below stay inside these ranges and needn't reach their ends.
All inputs are finite; a program needn't handle non-finite values.
Results may differ from the reference program's by a relative error of at most 0.0071.
Values may be sent and summed in bfloat16 or wider, within the bound.
A program may use at most 128 MiB of HBM per device.

```python
import math
import jax
import jax.numpy as jnp
from jax import lax

D = 1024
GRADES = 5
NQ = 4096
NC = 16384


def embed_pair(key):
    query_key = jax.random.fold_in(key, 11)
    cand_key = jax.random.fold_in(key, 12)
    candidates = jnp.clip(jax.random.normal(cand_key, (NC, D), jnp.float32), -5.0, 5.0)
    queries = jnp.clip(jax.random.normal(query_key, (NQ, D), jnp.float32), -5.0, 5.0)
    return (queries, candidates)


def draw_queries(key, part):
    queries, candidates = embed_pair(key)
    return queries.astype(jnp.bfloat16)


def draw_candidates(key, part):
    queries, candidates = embed_pair(key)
    return candidates.astype(jnp.bfloat16)


def draw_grades(key, part):
    kind_key = jax.random.fold_in(key, 21)
    single_key = jax.random.fold_in(key, 22)
    cell_key = jax.random.fold_in(key, 23)
    kinds = jax.random.randint(kind_key, (NQ, 1), 0, 16)
    single = jax.random.randint(single_key, (NQ, 1), 0, GRADES)
    cells = jax.random.randint(cell_key, (NQ, NC), 0, 60)
    spread = cells % GRADES
    upper = 1 + cells % 4
    middle = 2 + cells % 2
    lower = cells % 3
    grades = jnp.where(kinds == 0, upper, jnp.where(kinds == 1, middle, jnp.where(kinds == 2, single, jnp.where(kinds == 3, lower, spread))))
    return grades.astype(jnp.int32)


def steps_of(key, dims, split, smallest, high):
    factor_of, own = 1.0, jax.random.fold_in(key, 6)
    for position, shards_of in split:
        heights = jnp.exp(jax.random.uniform(jax.random.fold_in(own, position), (shards_of,), jnp.float32, smallest / len(split), high / len(split)))
        factor_of = factor_of * jnp.repeat(heights, dims[position] // shards_of).reshape([-1 if axis == position else 1 for axis in range(len(dims))])
    return factor_of


def noise(rng, dims, scale, limit, split=(), held_as=jnp.bfloat16):
    result = scale * jax.random.normal(rng, dims, jnp.float32)
    if split:
        result = result * steps_of(rng, dims, split, -0.22, 0.18)
    return jnp.clip(result, -limit, limit).astype(held_as)


def setup_inputs(seed: int = 0) -> dict:
    streams_of = jax.random.split(jax.random.key(seed), 5)
    return {
        "queries": draw_queries(jax.random.fold_in(streams_of[4], 71), 0),
        "candidates": draw_candidates(jax.random.fold_in(streams_of[4], 71), 0),
        "grades": draw_grades(jax.random.fold_in(streams_of[4], 71), 0),
        "query_weights": noise(streams_of[3], (NQ,), NC ** -0.5, 0.046875, ((0, 2),), jnp.float32),
    }


lowest = -1e+30

def grade_levels(maxima, masses, counts):
    levels = []
    running = maxima[0]
    seen_count = counts[0] * 0.0
    for bucket in range(len(maxima)):
        running = jnp.maximum(running, maxima[bucket])
        seen_count = seen_count + counts[bucket]
        summed = masses[0] * jnp.exp(maxima[0] - running)
        for lesser in range(1, bucket + 1):
            summed = summed + masses[lesser] * jnp.exp(maxima[lesser] - running)
        present = seen_count > 0.0
        levels.append(jnp.where(present, running + jnp.log(jnp.where(present, summed, 1.0)), running))
    return levels

def slope_factors(maxima, levels, counts):
    factors = []
    for bucket in range(len(maxima)):
        summed = counts[bucket] * jnp.exp(maxima[bucket] - levels[bucket])
        for higher in range(bucket + 1, len(maxima)):
            summed = summed + counts[higher] * jnp.exp(maxima[bucket] - levels[higher])
        factors.append(summed)
    return factors

def block_terms(scores, grade_block, weights):
    maxima, masses, counts = ([], [], [])
    for bucket in range(GRADES):
        member = grade_block == bucket
        highest = lax.optimization_barrier(jnp.max(jnp.where(member, scores, lowest), axis=1))
        masses.append(lax.optimization_barrier(jnp.sum(jnp.exp(jnp.where(member, scores - highest[:, None], lowest)), axis=1)))
        counts.append(lax.optimization_barrier(jnp.sum(member.astype(jnp.float32), axis=1)))
        maxima.append(highest)
    totals = lax.optimization_barrier(jnp.sum(scores, axis=1))
    levels = grade_levels(maxima, masses, counts)
    weighted = counts[0] * levels[0]
    for bucket in range(1, GRADES):
        weighted = weighted + counts[bucket] * levels[bucket]
    losses = (weighted - totals) / NC
    factors = slope_factors(maxima, levels, counts)
    picked_factor = jnp.zeros(scores.shape, jnp.float32)
    picked_max = jnp.zeros(scores.shape, jnp.float32)
    for bucket in range(GRADES):
        member = grade_block == bucket
        picked_factor = jnp.where(member, factors[bucket][:, None], picked_factor)
        picked_max = jnp.where(member, maxima[bucket][:, None], picked_max)
    slopes = (weights[:, None] * (picked_factor * jnp.exp(scores - picked_max) - 1.0)).astype(jnp.bfloat16)
    return (losses, slopes)

def reference(queries, candidates, grades, query_weights):
    scaling = 1.0 / math.sqrt(D)
    block_rows = math.gcd(NQ, 256)
    blocks = NQ // block_rows
    query_blocks = queries.reshape(blocks, block_rows, D)
    grade_blocks = grades.reshape(blocks, block_rows, NC)
    weight_blocks = query_weights.reshape(blocks, block_rows)

    def advance(cand_total, pieces):
        row_block, grade_block, weights = pieces
        scores = jnp.dot(row_block, candidates.T, preferred_element_type=jnp.float32) * scaling
        losses, slopes = block_terms(scores, grade_block, weights)
        query_part = (jnp.dot(slopes, candidates, preferred_element_type=jnp.float32) * scaling).astype(jnp.bfloat16)
        cand_total = cand_total + lax.dot_general(slopes, row_block, (((0,), (0,)), ((), ())), preferred_element_type=jnp.float32)
        return (cand_total, (losses, query_part))
    initial = jnp.zeros((NC, D), jnp.float32)
    final, (losses, query_parts) = lax.scan(advance, initial, (query_blocks, grade_blocks, weight_blocks))
    return (losses.reshape(NQ), query_parts.reshape(NQ, D), (final * scaling).astype(jnp.bfloat16))
```

```python
import functools
import math

import jax
import jax.numpy as jnp
from jax import lax
from jax.experimental import pallas as pl
from jax.experimental.pallas import tpu as pltpu
from jax.sharding import PartitionSpec as P

GRADES = 5
STATS = 16
LOWEST = -1e30
MESH = pl.DeviceIdType.MESH
F32 = jnp.float32
BF16 = jnp.bfloat16


def dev(p, i):
    return {"pb": p, "col": i}


class Place:
    def __init__(self, n_col, n_pb):
        self.n_col, self.n_pb = n_col, n_pb
        self.cores = 2 if n_col % 2 == 0 else 1
        rest = n_col // self.cores
        self.mids = 2 if rest % 2 == 0 else 1
        self.outs = rest // self.mids
        self.me = lax.axis_index("col")
        self.p = lax.axis_index("pb")
        self.core = lax.rem(self.me, self.cores)
        chip = self.me // self.cores
        self.mid = lax.rem(chip, self.mids)
        self.out = chip // self.mids

    def index(self, do, dm, dc):
        o = lax.rem(self.out + do, self.outs)
        m = lax.rem(self.mid + dm, self.mids)
        c = lax.rem(self.core + dc, self.cores)
        return (o * self.mids + m) * self.cores + c

    def peers(self):
        found = [dev(self.p, self.index(d, 0, 0)) for d in range(1, self.outs)]
        found += [dev(self.p, self.index(0, d, 0)) for d in range(1, self.mids)]
        found += [dev(self.p, self.index(0, 0, d)) for d in range(1, self.cores)]
        found += [dev(lax.rem(self.p + d, self.n_pb), self.me) for d in range(1, self.n_pb)]
        return found


def greet(peers):
    barrier = pltpu.get_barrier_semaphore()
    for peer in peers:
        pl.semaphore_signal(barrier, inc=1, device_id=peer, device_id_type=MESH)
    pl.semaphore_wait(barrier, len(peers))


def remote(src, dst, send, recv, device):
    return pltpu.make_async_remote_copy(
        src_ref=src, dst_ref=dst, send_sem=send, recv_sem=recv, device_id=device, device_id_type=MESH
    )


def gather_kernel(n_col, n_pb, q_ref, c_ref, q_all, c_all, q_send, q_recv, c_send, c_recv, own_sem):
    at = Place(n_col, n_pb)
    own = [
        pltpu.make_async_copy(q_ref, q_all.at[at.me], own_sem.at[0]),
        pltpu.make_async_copy(c_ref, c_all.at[at.p], own_sem.at[1]),
    ]
    for copy in own:
        copy.start()
    greet(at.peers())
    c_copies = []
    for d in range(1, n_pb):
        other = lax.rem(at.p + d, n_pb)
        copy = remote(c_ref, c_all.at[at.p], c_send.at[d], c_recv.at[at.p], dev(other, at.me))
        copy.start()
        c_copies.append(copy)
    sends = []

    def push(src, block, device):
        copy = remote(src, q_all.at[block], q_send.at[len(sends)], q_recv.at[block], device)
        copy.start()
        sends.append(copy)

    def arrived(block):
        remote(q_ref, q_all.at[block], q_send.at[0], q_recv.at[block], dev(at.p, at.me)).wait_recv()

    def spread(do, dm):
        block = at.index(do, dm, 0)
        if do or dm:
            arrived(block)
            src = q_all.at[block]
        else:
            src = q_ref
        if dm == 0:
            if do == 0:
                for d in range(1, at.outs):
                    push(src, block, dev(at.p, at.index(d, 0, 0)))
            for d in range(1, at.mids):
                push(src, block, dev(at.p, at.index(0, d, 0)))
        for d in range(1, at.cores):
            push(src, block, dev(at.p, at.index(0, 0, d)))

    order = [0] + sorted(range(1, at.outs), key=lambda d: min(d, at.outs - d))
    for do in order:
        spread(do, 0)
    for do in order:
        for dm in range(1, at.mids):
            spread(do, dm)
    for d in range(1, at.cores):
        for do in order:
            for dm in range(at.mids):
                arrived(at.index(do, dm, d))
    for d in range(1, n_pb):
        other = lax.rem(at.p + d, n_pb)
        remote(c_ref, c_all.at[other], c_send.at[0], c_recv.at[other], dev(at.p, at.me)).wait_recv()
    for copy in sends + c_copies:
        copy.wait_send()
    for copy in own:
        copy.wait()


def gather(q, c, n_col, n_pb):
    vmem = pl.BlockSpec(memory_space=pltpu.VMEM)
    hbm = pl.BlockSpec(memory_space=pl.ANY)
    return pl.pallas_call(
        functools.partial(gather_kernel, n_col, n_pb),
        out_shape=(
            jax.ShapeDtypeStruct((n_col, *q.shape), q.dtype),
            jax.ShapeDtypeStruct((n_pb, *c.shape), c.dtype),
        ),
        in_specs=[vmem, vmem],
        out_specs=(hbm, hbm),
        scratch_shapes=[
            pltpu.SemaphoreType.DMA((2 * n_col,)),
            pltpu.SemaphoreType.DMA((n_col,)),
            pltpu.SemaphoreType.DMA((n_pb,)),
            pltpu.SemaphoreType.DMA((n_pb,)),
            pltpu.SemaphoreType.DMA((2,)),
        ],
        compiler_params=pltpu.CompilerParams(collective_id=0, has_side_effects=True),
        name="gather",
    )(q, c)


def score_kernel(scaling, q_ref, c_ref, g_ref, e_ref, s_ref):
    rows = g_ref.shape[0]
    scores = (
        lax.dot_general(
            q_ref[0], c_ref[...], (((1,), (1,)), ((), ())), preferred_element_type=F32
        )
        * scaling
    )
    grades = g_ref[...]
    lane = lax.broadcasted_iota(jnp.int32, (rows, rows), 1)
    table = jnp.zeros((rows, rows), F32)
    picked = jnp.zeros(scores.shape, F32)
    for b in range(GRADES):
        member = grades == b
        highest = jnp.max(jnp.where(member, scores, LOWEST), axis=1, keepdims=True)
        picked = jnp.where(member, highest, picked)
        table = jnp.where(lane == b, highest, table)
    expo = jnp.exp(scores - picked)
    e_ref[...] = expo
    for b in range(GRADES):
        member = grades == b
        mass = jnp.sum(jnp.where(member, expo, 0.0), axis=1, keepdims=True)
        count = jnp.sum(jnp.where(member, 1.0, 0.0), axis=1, keepdims=True)
        table = jnp.where(lane == GRADES + b, mass, table)
        table = jnp.where(lane == 2 * GRADES + b, count, table)
    total = jnp.sum(scores, axis=1, keepdims=True)
    table = jnp.where(lane == 3 * GRADES, total, table)
    s_ref[0] = table.T[:STATS]


def score(q_all, c_block, grades, scaling):
    n, rows, width = q_all.shape
    cols = c_block.shape[0]
    return pl.pallas_call(
        functools.partial(score_kernel, scaling),
        grid=(n,),
        out_shape=(
            jax.ShapeDtypeStruct(grades.shape, F32),
            jax.ShapeDtypeStruct((n, STATS, rows), F32),
        ),
        in_specs=[
            pl.BlockSpec((1, rows, width), lambda i: (i, 0, 0)),
            pl.BlockSpec((cols, width), lambda i: (0, 0)),
            pl.BlockSpec((rows, cols), lambda i: (i, 0)),
        ],
        out_specs=(
            pl.BlockSpec((rows, cols), lambda i: (i, 0)),
            pl.BlockSpec((1, STATS, rows), lambda i: (i, 0, 0)),
        ),
        compiler_params=pltpu.CompilerParams(vmem_limit_bytes=40 * 2**20),
        name="score",
    )(q_all, c_block, grades)


def merge_kernel(n_col, columns, s_ref, all_ref, got, mine, send, recv, send2, recv2):
    me = lax.axis_index("col")
    p = lax.axis_index("pb")
    others = [lax.rem(me + d, n_col) for d in range(1, n_col)]
    greet([dev(p, o) for o in others])
    copies = []
    for d, o in enumerate(others):
        copy = remote(s_ref.at[o], got.at[me], send.at[d], recv.at[me], dev(p, o))
        copy.start()
        copies.append(copy)
    got[me] = s_ref[me]
    for o in others:
        remote(s_ref.at[o], got.at[o], send.at[0], recv.at[o], dev(p, o)).wait_recv()
    G = GRADES
    maxima = got[0][:G]
    for k in range(1, n_col):
        maxima = jnp.maximum(maxima, got[k][:G])
    masses = jnp.zeros_like(maxima)
    rest = jnp.zeros((STATS - 2 * G, maxima.shape[1]), F32)
    for k in range(n_col):
        block = got[k]
        masses = masses + block[G : 2 * G] * jnp.exp(block[:G] - maxima)
        rest = rest + block[2 * G :]
    mx = [maxima[b : b + 1] for b in range(G)]
    ms = [masses[b : b + 1] for b in range(G)]
    ct = [rest[b : b + 1] for b in range(G)]
    total = rest[G : G + 1]
    levels = []
    running = mx[0]
    seen = ct[0] * 0.0
    for b in range(G):
        running = jnp.maximum(running, mx[b])
        seen = seen + ct[b]
        summed = ms[0] * jnp.exp(mx[0] - running)
        for h in range(1, b + 1):
            summed = summed + ms[h] * jnp.exp(mx[h] - running)
        present = seen > 0.0
        levels.append(jnp.where(present, running + jnp.log(jnp.where(present, summed, 1.0)), running))
    weighted = ct[0] * levels[0]
    for b in range(1, G):
        weighted = weighted + ct[b] * levels[b]
    loss = (weighted - total) / columns
    factors = []
    for h in range(G):
        f = ct[h] * jnp.exp(mx[h] - levels[h])
        for b in range(h + 1, G):
            f = f + ct[b] * jnp.exp(mx[h] - levels[b])
        factors.append(f)
    pad = jnp.zeros((STATS - 2 * G - 1, loss.shape[1]), F32)
    mine[...] = jnp.concatenate(mx + factors + [loss, pad], axis=0)
    more = []
    for d, o in enumerate(others):
        copy = remote(mine, all_ref.at[me], send2.at[d], recv2.at[me], dev(p, o))
        copy.start()
        more.append(copy)
    all_ref[me] = mine[...]
    for o in others:
        remote(mine, all_ref.at[o], send2.at[0], recv2.at[o], dev(p, o)).wait_recv()
    for copy in copies + more:
        copy.wait_send()


def merge(stats, columns):
    n_col, _, rows = stats.shape
    vmem = pl.BlockSpec(memory_space=pltpu.VMEM)
    return pl.pallas_call(
        functools.partial(merge_kernel, n_col, columns),
        out_shape=jax.ShapeDtypeStruct(stats.shape, F32),
        in_specs=[vmem],
        out_specs=vmem,
        scratch_shapes=[
            pltpu.VMEM(stats.shape, F32),
            pltpu.VMEM((STATS, rows), F32),
            pltpu.SemaphoreType.DMA((n_col,)),
            pltpu.SemaphoreType.DMA((n_col,)),
            pltpu.SemaphoreType.DMA((n_col,)),
            pltpu.SemaphoreType.DMA((n_col,)),
        ],
        compiler_params=pltpu.CompilerParams(collective_id=1, has_side_effects=True),
        name="merge",
    )(stats)


def slope_kernel(scaling, per, e_ref, g_ref, q_ref, c_ref, s_ref, f_ref, w_ref, qg_ref, cg_ref, acc):
    step = pl.program_id(0)
    G = GRADES
    rows = s_ref.shape[2]
    pieces = []
    for k in range(per):
        local, merged, weight = s_ref[k], f_ref[k], w_ref[k]
        scaled = weight * (merged[G : 2 * G] * jnp.exp(local[:G] - merged[:G]))
        table = jnp.concatenate([scaled, weight, jnp.zeros((rows - G - 1, rows), F32)], axis=0).T
        grades = g_ref[k * rows : (k + 1) * rows]
        picked = jnp.broadcast_to(table[:, 0:1], grades.shape)
        for b in range(1, G):
            picked = jnp.where(grades == b, table[:, b : b + 1], picked)
        slopes = picked * e_ref[k * rows : (k + 1) * rows] - table[:, G : G + 1]
        pieces.append(slopes.astype(BF16))
    slopes = jnp.concatenate(pieces, axis=0)
    part = jnp.dot(slopes, c_ref[...], preferred_element_type=F32) * scaling
    qg_ref[...] = part.astype(BF16).reshape(qg_ref.shape)
    term = lax.dot_general(
        slopes,
        q_ref[...].reshape(per * rows, -1),
        (((0,), (0,)), ((), ())),
        preferred_element_type=F32,
    )

    @pl.when(step == 0)
    def _():
        acc[...] = term

    @pl.when(step > 0)
    def _():
        acc[...] += term

    @pl.when(step == pl.num_programs(0) - 1)
    def _():
        cg_ref[...] = (acc[...] * scaling).astype(BF16)


def slope(expo, grades, q_all, c_block, stats, merged, weights, scaling):
    n, rows, width = q_all.shape
    cols = c_block.shape[0]
    per = 2 if n % 2 == 0 else 1
    block3 = lambda a, b: pl.BlockSpec((per, a, b), lambda i: (i, 0, 0))
    return pl.pallas_call(
        functools.partial(slope_kernel, scaling, per),
        grid=(n // per,),
        out_shape=(
            jax.ShapeDtypeStruct((n, rows, width), BF16),
            jax.ShapeDtypeStruct((cols, width), BF16),
        ),
        in_specs=[
            pl.BlockSpec((per * rows, cols), lambda i: (i, 0)),
            pl.BlockSpec((per * rows, cols), lambda i: (i, 0)),
            block3(rows, width),
            pl.BlockSpec((cols, width), lambda i: (0, 0)),
            block3(STATS, rows),
            block3(STATS, rows),
            block3(1, rows),
        ],
        out_specs=(block3(rows, width), pl.BlockSpec((cols, width), lambda i: (0, 0))),
        scratch_shapes=[pltpu.VMEM((cols, width), F32)],
        compiler_params=pltpu.CompilerParams(vmem_limit_bytes=48 * 2**20),
        name="slope",
    )(expo, grades, q_all, c_block, stats, merged, weights)


def scatter_kernel(
    n_col, n_pb, qg, cg, q_out, c_out,
    core_got, acc, mid_got, out_got, c_got,
    core_send, core_recv, mid_send, mid_recv, out_send, out_recv, c_send, c_recv,
):
    at = Place(n_col, n_pb)
    greet(at.peers())
    copies = []

    def push(*args):
        copy = remote(*args)
        copy.start()
        copies.append(copy)

    for d in range(1, n_pb):
        other = lax.rem(at.p + d, n_pb)
        push(cg.at[other], c_got.at[d - 1], c_send.at[d], c_recv.at[d - 1], dev(other, at.me))
    order = sorted(range(1, at.outs), key=lambda d: min(d, at.outs - d)) + [0]
    far = [(do, dm) for do in order for dm in range(1, at.mids)] + [(do, 0) for do in order]
    slot = {pair: k for k, pair in enumerate(far)}
    for do, dm in far:
        k = slot[do, dm]
        if at.cores > 1:
            push(
                qg.at[at.index(do, dm, 1)], core_got.at[k], core_send.at[k], core_recv.at[k],
                dev(at.p, at.index(0, 0, 1)),
            )

    def core_sum(do, dm):
        k = slot[do, dm]
        own = qg[at.index(do, dm, 0)].astype(F32)
        if at.cores > 1:
            remote(core_got.at[k], core_got.at[k], core_send.at[k], core_recv.at[k], dev(at.p, at.me)).wait_recv()
            own = own + core_got[k].astype(F32)
        return own

    for do in order:
        for dm in range(1, at.mids):
            k = slot[do, dm]
            acc[k] = core_sum(do, dm).astype(BF16)
            push(acc.at[k], mid_got.at[k], mid_send.at[k], mid_recv.at[k], dev(at.p, at.index(0, dm, 0)))
    for do in order:
        k = slot[do, 0]
        acc[k] = core_sum(do, 0).astype(BF16)
    for do in order:
        k = slot[do, 0]
        total = acc[k].astype(F32)
        for dm in range(1, at.mids):
            j = slot[do, dm]
            remote(acc.at[j], mid_got.at[j], mid_send.at[j], mid_recv.at[j], dev(at.p, at.me)).wait_recv()
            total = total + mid_got[j].astype(F32)
        if do:
            acc[k] = total.astype(BF16)
            push(acc.at[k], out_got.at[do - 1], out_send.at[do - 1], out_recv.at[do - 1], dev(at.p, at.index(do, 0, 0)))
    for d in range(1, at.outs):
        remote(acc.at[0], out_got.at[d - 1], out_send.at[d - 1], out_recv.at[d - 1], dev(at.p, at.me)).wait_recv()
        total = total + out_got[d - 1].astype(F32)
    q_out[...] = total.astype(BF16)
    for d in range(1, n_pb):
        remote(cg.at[0], c_got.at[d - 1], c_send.at[d], c_recv.at[d - 1], dev(at.p, at.me)).wait_recv()
    half = 128
    for r in range(0, c_out.shape[0], half):
        rows = pl.ds(r, half)
        c_total = cg[at.p, rows].astype(F32)
        for d in range(1, n_pb):
            c_total = c_total + c_got[d - 1, rows].astype(F32)
        c_out[rows] = c_total.astype(BF16)
    for copy in copies:
        copy.wait_send()


def scatter(qg, cg):
    n_col, rows, width = qg.shape
    n_pb, crows, _ = cg.shape
    vmem = pl.BlockSpec(memory_space=pltpu.VMEM)
    block = (rows, width)
    dma = pltpu.SemaphoreType.DMA
    return pl.pallas_call(
        functools.partial(scatter_kernel, n_col, n_pb),
        out_shape=(jax.ShapeDtypeStruct(block, BF16), jax.ShapeDtypeStruct((crows, width), BF16)),
        in_specs=[vmem, vmem],
        out_specs=(vmem, vmem),
        scratch_shapes=[
            pltpu.VMEM((n_col, *block), BF16),
            pltpu.VMEM((n_col, *block), BF16),
            pltpu.VMEM((n_col, *block), BF16),
            pltpu.VMEM((n_col, *block), BF16),
            pltpu.VMEM((max(n_pb - 1, 1), crows, width), BF16),
        ]
        + [dma((n_col,))] * 6
        + [dma((n_pb,))] * 2,
        compiler_params=pltpu.CompilerParams(
            collective_id=2, has_side_effects=True, vmem_limit_bytes=60 * 2**20
        ),
        name="scatter",
    )(qg, cg)


def local(queries, candidates, grades, query_weights):
    n_col, n_pb = lax.axis_size("col"), lax.axis_size("pb")
    width = queries.shape[1]
    rows = queries.shape[0]
    scaling = 1.0 / math.sqrt(width)
    q_all, c_all = gather(queries, candidates, n_col, n_pb)
    c_block = c_all.reshape(-1, width)
    expo, stats = score(q_all, c_block, grades, scaling)
    merged = merge(stats, grades.shape[1] * n_col)
    losses = merged[:, 2 * GRADES].reshape(-1)
    weights = query_weights.reshape(n_col, 1, rows)
    qg, cg = slope(expo, grades, q_all, c_block, stats, merged, weights, scaling)
    query_grad, cand_grad = scatter(qg, cg.reshape(n_pb, -1, width))
    return (losses, query_grad, cand_grad)


def solution(mesh):
    in_specs = (P(("pb", "col"), None), P(("col", "pb"), None), P("pb", "col"), P("pb"))
    out_specs = (P("pb"), P(("pb", "col"), None), P(("col", "pb"), None))
    return jax.shard_map(local, mesh=mesh, in_specs=in_specs, out_specs=out_specs, check_vma=False)
```

```python
import functools
import math

import jax
import jax.numpy as jnp
from jax import lax
from jax.experimental import pallas as pl
from jax.experimental.pallas import tpu as pltpu
from jax.sharding import PartitionSpec as P

GRADES = 5
STATS = 16
LOWEST = -1e30
MESH = pl.DeviceIdType.MESH
F32 = jnp.float32
BF16 = jnp.bfloat16


def dev(p, i):
    return {"pb": p, "col": i}


class Place:
    def __init__(self, n_col, n_pb):
        self.n_col, self.n_pb = n_col, n_pb
        self.cores = 2 if n_col % 2 == 0 else 1
        rest = n_col // self.cores
        self.mids = 2 if rest % 2 == 0 else 1
        self.outs = rest // self.mids
        self.me = lax.axis_index("col")
        self.p = lax.axis_index("pb")
        self.core = lax.rem(self.me, self.cores)
        chip = self.me // self.cores
        self.mid = lax.rem(chip, self.mids)
        self.out = chip // self.mids

    def index(self, do, dm, dc):
        o = lax.rem(self.out + do, self.outs)
        m = lax.rem(self.mid + dm, self.mids)
        c = lax.rem(self.core + dc, self.cores)
        return (o * self.mids + m) * self.cores + c

    def peers(self):
        found = [dev(self.p, self.index(d, 0, 0)) for d in range(1, self.outs)]
        found += [dev(self.p, self.index(0, d, 0)) for d in range(1, self.mids)]
        found += [dev(self.p, self.index(0, 0, d)) for d in range(1, self.cores)]
        found += [dev(lax.rem(self.p + d, self.n_pb), self.me) for d in range(1, self.n_pb)]
        return found


def greet(peers):
    barrier = pltpu.get_barrier_semaphore()
    for peer in peers:
        pl.semaphore_signal(barrier, inc=1, device_id=peer, device_id_type=MESH)
    pl.semaphore_wait(barrier, len(peers))


def remote(src, dst, send, recv, device):
    return pltpu.make_async_remote_copy(
        src_ref=src, dst_ref=dst, send_sem=send, recv_sem=recv, device_id=device, device_id_type=MESH
    )


def score_tile(scaling, q, c, grades):
    rows = grades.shape[0]
    scores = lax.dot_general(q, c, (((1,), (1,)), ((), ())), preferred_element_type=F32) * scaling
    lane = lax.broadcasted_iota(jnp.int32, (rows, rows), 1)
    table = jnp.zeros((rows, rows), F32)
    picked = jnp.zeros(scores.shape, F32)
    for b in range(GRADES):
        member = grades == b
        highest = jnp.max(jnp.where(member, scores, LOWEST), axis=1, keepdims=True)
        picked = jnp.where(member, highest, picked)
        table = jnp.where(lane == b, highest, table)
    expo = jnp.exp(scores - picked)
    for b in range(GRADES):
        member = grades == b
        mass = jnp.sum(jnp.where(member, expo, 0.0), axis=1, keepdims=True)
        count = jnp.sum(jnp.where(member, 1.0, 0.0), axis=1, keepdims=True)
        table = jnp.where(lane == GRADES + b, mass, table)
        table = jnp.where(lane == 2 * GRADES + b, count, table)
    total = jnp.sum(scores, axis=1, keepdims=True)
    table = jnp.where(lane == 3 * GRADES, total, table)
    return expo, table.T[:STATS]


def front_kernel(
    n_col, n_pb, scaling, q_ref, c_ref, g_hbm, q_all, c_all, e_hbm, s_all,
    g_all, e_all, q_send, q_recv, c_send, c_recv, own_sem, e_sem,
):
    at = Place(n_col, n_pb)
    rows, half = q_ref.shape[0], c_ref.shape[0]
    grades_in = pltpu.make_async_copy(g_hbm, g_all, own_sem.at[0])
    grades_in.start()
    own = [
        pltpu.make_async_copy(q_ref, q_all.at[at.me], own_sem.at[1]),
        pltpu.make_async_copy(c_ref, c_all.at[at.p], own_sem.at[2]),
    ]
    for copy in own:
        copy.start()
    greet(at.peers())
    c_copies = []
    for d in range(1, n_pb):
        other = lax.rem(at.p + d, n_pb)
        copy = remote(c_ref, c_all.at[at.p], c_send.at[d], c_recv.at[at.p], dev(other, at.me))
        copy.start()
        c_copies.append(copy)
    sends = []

    def push(src, block, device):
        copy = remote(src, q_all.at[block], q_send.at[len(sends)], q_recv.at[block], device)
        copy.start()
        sends.append(copy)

    def arrived(block):
        remote(q_ref, q_all.at[block], q_send.at[0], q_recv.at[block], dev(at.p, at.me)).wait_recv()

    def forward(do, dm):
        block = at.index(do, dm, 0)
        src = q_ref
        if do or dm:
            arrived(block)
            src = q_all.at[block]
        if dm == 0:
            if do == 0:
                for d in order[1:]:
                    push(src, block, dev(at.p, at.index(d, 0, 0)))
            for d in range(1, at.mids):
                push(src, block, dev(at.p, at.index(0, d, 0)))
        for d in range(1, at.cores):
            push(src, block, dev(at.p, at.index(0, 0, d)))

    def task(block, part):
        span = pl.ds(pl.multiple_of(block * rows, rows), rows)
        columns = pl.ds(pl.multiple_of(part * half, half), half)
        expo, stats = score_tile(scaling, q_all[block], c_all[part], g_all[span, columns])
        e_all[block, part] = expo
        s_all[block, part] = stats
        pltpu.make_async_copy(
            e_all.at[block, part], e_hbm.at[block, part], e_sem.at[block, part]
        ).start()

    order = [0] + sorted(range(1, at.outs), key=lambda d: min(d, at.outs - d))
    last = order[-1]

    def group(pairs):
        first = pairs[0]
        step = [b - a for a, b in zip(first, pairs[-1])]

        def body(j, carry):
            which = j // at.cores
            dc = lax.rem(j, at.cores)
            block = at.index(first[0] + which * step[0], first[1] + which * step[1], dc)

            @pl.when(dc > 0)
            def _():
                arrived(block)

            task(block, at.p)
            return carry

        lax.fori_loop(0, len(pairs) * at.cores, body, 0)

    for k in range(at.outs):
        pairs = [(order[k], 0)]
        if k > 0 and at.mids > 1:
            pairs.append((order[k - 1], 1))
        for pair in pairs:
            forward(*pair)
        if k == 0:
            for copy in own:
                copy.wait()
            grades_in.wait()
        group(pairs)

    def later(first, count):
        for d in range(1, n_pb):
            part = lax.rem(at.p + d, n_pb)

            def body(j, carry):
                do = last + 1 + j // (at.mids * at.cores)
                dm = lax.rem(j // at.cores, at.mids)
                task(at.index(do, dm, lax.rem(j, at.cores)), part)
                return carry

            if first == 0:
                remote(
                    c_ref, c_all.at[part], c_send.at[0], c_recv.at[part], dev(at.p, at.me)
                ).wait_recv()
            lax.fori_loop(first, first + count, body, 0)

    tail = at.cores if at.mids > 1 else 0
    if tail:
        forward(last, 1)
    later(0, n_col - tail)
    if tail:
        group([(last, 1)])
        later(n_col - tail, tail)

    def drain(j, carry):
        for part in range(n_pb):
            pltpu.make_async_copy(e_all.at[j, part], e_hbm.at[j, part], e_sem.at[j, part]).wait()
        return carry

    lax.fori_loop(0, n_col, drain, 0)
    for copy in sends + c_copies:
        copy.wait_send()


def front(q, c, grades, n_col, n_pb, scaling):
    vmem = pl.BlockSpec(memory_space=pltpu.VMEM)
    hbm = pl.BlockSpec(memory_space=pl.ANY)
    rows, half = q.shape[0], c.shape[0]
    e_shape = (n_col, n_pb, rows, half)
    dma = pltpu.SemaphoreType.DMA
    return pl.pallas_call(
        functools.partial(front_kernel, n_col, n_pb, scaling),
        out_shape=(
            jax.ShapeDtypeStruct((n_col, *q.shape), q.dtype),
            jax.ShapeDtypeStruct((n_pb, *c.shape), c.dtype),
            jax.ShapeDtypeStruct(e_shape, F32),
            jax.ShapeDtypeStruct((n_col, n_pb, STATS, rows), F32),
        ),
        in_specs=[vmem, vmem, hbm],
        out_specs=(vmem, vmem, hbm, vmem),
        scratch_shapes=[
            pltpu.VMEM(grades.shape, jnp.int32),
            pltpu.VMEM(e_shape, F32),
            dma((2 * n_col,)),
            dma((n_col,)),
            dma((n_pb,)),
            dma((n_pb,)),
            dma((3,)),
            dma((n_col, n_pb)),
        ],
        compiler_params=pltpu.CompilerParams(
            collective_id=0, has_side_effects=True, vmem_limit_bytes=56 * 2**20
        ),
        name="front",
    )(q, c, grades)


def merge_kernel(n_col, columns, parts_ref, all_ref, s_ref, got, mine, send, recv, send2, recv2):
    me = lax.axis_index("col")
    p = lax.axis_index("pb")
    others = [lax.rem(me + d, n_col) for d in range(1, n_col)]
    greet([dev(p, o) for o in others])
    G = GRADES
    for k in range(n_col):
        parts = [parts_ref[k, h] for h in range(parts_ref.shape[1])]
        top = parts[0][:G]
        for part in parts[1:]:
            top = jnp.maximum(top, part[:G])
        mass = sum(part[G : 2 * G] * jnp.exp(part[:G] - top) for part in parts)
        s_ref[k] = jnp.concatenate([top, mass, sum(part[2 * G :] for part in parts)], axis=0)
    copies = []
    for d, o in enumerate(others):
        copy = remote(s_ref.at[o], got.at[me], send.at[d], recv.at[me], dev(p, o))
        copy.start()
        copies.append(copy)
    got[me] = s_ref[me]
    for o in others:
        remote(s_ref.at[o], got.at[o], send.at[0], recv.at[o], dev(p, o)).wait_recv()
    maxima = got[0][:G]
    for k in range(1, n_col):
        maxima = jnp.maximum(maxima, got[k][:G])
    masses = jnp.zeros_like(maxima)
    rest = jnp.zeros((STATS - 2 * G, maxima.shape[1]), F32)
    for k in range(n_col):
        block = got[k]
        masses = masses + block[G : 2 * G] * jnp.exp(block[:G] - maxima)
        rest = rest + block[2 * G :]
    mx = [maxima[b : b + 1] for b in range(G)]
    ms = [masses[b : b + 1] for b in range(G)]
    ct = [rest[b : b + 1] for b in range(G)]
    total = rest[G : G + 1]
    levels = []
    running = mx[0]
    seen = ct[0] * 0.0
    for b in range(G):
        running = jnp.maximum(running, mx[b])
        seen = seen + ct[b]
        summed = ms[0] * jnp.exp(mx[0] - running)
        for h in range(1, b + 1):
            summed = summed + ms[h] * jnp.exp(mx[h] - running)
        present = seen > 0.0
        levels.append(jnp.where(present, running + jnp.log(jnp.where(present, summed, 1.0)), running))
    weighted = ct[0] * levels[0]
    for b in range(1, G):
        weighted = weighted + ct[b] * levels[b]
    loss = (weighted - total) / columns
    factors = []
    for h in range(G):
        f = ct[h] * jnp.exp(mx[h] - levels[h])
        for b in range(h + 1, G):
            f = f + ct[b] * jnp.exp(mx[h] - levels[b])
        factors.append(f)
    pad = jnp.zeros((STATS - 2 * G - 1, loss.shape[1]), F32)
    mine[...] = jnp.concatenate(mx + factors + [loss, pad], axis=0)
    more = []
    for d, o in enumerate(others):
        copy = remote(mine, all_ref.at[me], send2.at[d], recv2.at[me], dev(p, o))
        copy.start()
        more.append(copy)
    all_ref[me] = mine[...]
    for o in others:
        remote(mine, all_ref.at[o], send2.at[0], recv2.at[o], dev(p, o)).wait_recv()
    for copy in copies + more:
        copy.wait_send()


def merge(stats, columns):
    n_col, _, _, rows = stats.shape
    shape = (n_col, STATS, rows)
    vmem = pl.BlockSpec(memory_space=pltpu.VMEM)
    return pl.pallas_call(
        functools.partial(merge_kernel, n_col, columns),
        out_shape=jax.ShapeDtypeStruct(shape, F32),
        in_specs=[vmem],
        out_specs=vmem,
        scratch_shapes=[
            pltpu.VMEM(shape, F32),
            pltpu.VMEM(shape, F32),
            pltpu.VMEM((STATS, rows), F32),
            pltpu.SemaphoreType.DMA((n_col,)),
            pltpu.SemaphoreType.DMA((n_col,)),
            pltpu.SemaphoreType.DMA((n_col,)),
            pltpu.SemaphoreType.DMA((n_col,)),
        ],
        compiler_params=pltpu.CompilerParams(collective_id=1, has_side_effects=True),
        name="merge",
    )(stats)


def slope_kernel(scaling, per, e_ref, g_ref, q_ref, c_ref, s_ref, f_ref, w_ref, qg_ref, cg_ref, acc):
    step = pl.program_id(0)
    G = GRADES
    rows = s_ref.shape[3]
    pieces = []
    n_pb = s_ref.shape[1]
    half = e_ref.shape[3]
    for k in range(per):
        merged, weight = f_ref[k], w_ref[k]
        factor = weight * merged[G : 2 * G]
        scaled = [factor * jnp.exp(s_ref[k, h, :G] - merged[:G]) for h in range(n_pb)]
        pad = jnp.zeros((rows - n_pb * G - 1, rows), F32)
        table = jnp.concatenate(scaled + [weight, pad], axis=0).T
        sections = []
        for h in range(n_pb):
            grades = g_ref[k * rows : (k + 1) * rows, h * half : (h + 1) * half]
            picked = jnp.broadcast_to(table[:, h * G : h * G + 1], grades.shape)
            for b in range(1, G):
                picked = jnp.where(grades == b, table[:, h * G + b : h * G + b + 1], picked)
            sections.append(picked * e_ref[k, h] - table[:, n_pb * G : n_pb * G + 1])
        slopes = jnp.concatenate(sections, axis=1)
        pieces.append(slopes.astype(BF16))
    slopes = jnp.concatenate(pieces, axis=0)
    part = jnp.dot(slopes, c_ref[...], preferred_element_type=F32) * scaling
    qg_ref[...] = part.astype(BF16).reshape(qg_ref.shape)
    term = lax.dot_general(
        slopes,
        q_ref[...].reshape(per * rows, -1),
        (((0,), (0,)), ((), ())),
        preferred_element_type=F32,
    )

    @pl.when(step == 0)
    def _():
        acc[...] = term

    @pl.when(step > 0)
    def _():
        acc[...] += term

    @pl.when(step == pl.num_programs(0) - 1)
    def _():
        cg_ref[...] = (acc[...] * scaling).astype(BF16)


def slope(expo, grades, q_all, c_block, stats, merged, weights, scaling):
    n, rows, width = q_all.shape
    cols = c_block.shape[0]
    per = 2 if n % 2 == 0 else 1
    block3 = lambda a, b: pl.BlockSpec((per, a, b), lambda i: (i, 0, 0))
    block4 = lambda a, b, c: pl.BlockSpec((per, a, b, c), lambda i: (i, 0, 0, 0))
    return pl.pallas_call(
        functools.partial(slope_kernel, scaling, per),
        grid=(n // per,),
        out_shape=(
            jax.ShapeDtypeStruct((n, rows, width), BF16),
            jax.ShapeDtypeStruct((cols, width), BF16),
        ),
        in_specs=[
            block4(*expo.shape[1:]),
            pl.BlockSpec((per * rows, cols), lambda i: (i, 0)),
            block3(rows, width),
            pl.BlockSpec((cols, width), lambda i: (0, 0)),
            block4(*stats.shape[1:]),
            block3(STATS, rows),
            block3(1, rows),
        ],
        out_specs=(block3(rows, width), pl.BlockSpec((cols, width), lambda i: (0, 0))),
        scratch_shapes=[pltpu.VMEM((cols, width), F32)],
        compiler_params=pltpu.CompilerParams(vmem_limit_bytes=48 * 2**20),
        name="slope",
    )(expo, grades, q_all, c_block, stats, merged, weights)


def scatter_kernel(
    n_col, n_pb, qg, cg, q_out, c_out,
    core_got, acc, mid_got, out_got, c_got,
    core_send, core_recv, mid_send, mid_recv, out_send, out_recv, c_send, c_recv,
):
    at = Place(n_col, n_pb)
    greet(at.peers())
    copies = []

    def push(*args):
        copy = remote(*args)
        copy.start()
        copies.append(copy)

    for d in range(1, n_pb):
        other = lax.rem(at.p + d, n_pb)
        push(cg.at[other], c_got.at[d - 1], c_send.at[d], c_recv.at[d - 1], dev(other, at.me))
    order = sorted(range(1, at.outs), key=lambda d: min(d, at.outs - d)) + [0]
    far = [(do, dm) for do in order for dm in range(1, at.mids)] + [(do, 0) for do in order]
    slot = {pair: k for k, pair in enumerate(far)}
    for do, dm in far:
        k = slot[do, dm]
        if at.cores > 1:
            push(
                qg.at[at.index(do, dm, 1)], core_got.at[k], core_send.at[k], core_recv.at[k],
                dev(at.p, at.index(0, 0, 1)),
            )

    def core_sum(do, dm):
        k = slot[do, dm]
        own = qg[at.index(do, dm, 0)].astype(F32)
        if at.cores > 1:
            remote(core_got.at[k], core_got.at[k], core_send.at[k], core_recv.at[k], dev(at.p, at.me)).wait_recv()
            own = own + core_got[k].astype(F32)
        return own

    for do in order:
        for dm in range(1, at.mids):
            k = slot[do, dm]
            acc[k] = core_sum(do, dm).astype(BF16)
            push(acc.at[k], mid_got.at[k], mid_send.at[k], mid_recv.at[k], dev(at.p, at.index(0, dm, 0)))
    for do in order:
        k = slot[do, 0]
        acc[k] = core_sum(do, 0).astype(BF16)
    for do in order:
        k = slot[do, 0]
        total = acc[k].astype(F32)
        for dm in range(1, at.mids):
            j = slot[do, dm]
            remote(acc.at[j], mid_got.at[j], mid_send.at[j], mid_recv.at[j], dev(at.p, at.me)).wait_recv()
            total = total + mid_got[j].astype(F32)
        if do:
            acc[k] = total.astype(BF16)
            push(acc.at[k], out_got.at[do - 1], out_send.at[do - 1], out_recv.at[do - 1], dev(at.p, at.index(do, 0, 0)))
    for d in range(1, at.outs):
        remote(acc.at[0], out_got.at[d - 1], out_send.at[d - 1], out_recv.at[d - 1], dev(at.p, at.me)).wait_recv()
        total = total + out_got[d - 1].astype(F32)
    q_out[...] = total.astype(BF16)
    for d in range(1, n_pb):
        remote(cg.at[0], c_got.at[d - 1], c_send.at[d], c_recv.at[d - 1], dev(at.p, at.me)).wait_recv()
    half = 128
    for r in range(0, c_out.shape[0], half):
        rows = pl.ds(r, half)
        c_total = cg[at.p, rows].astype(F32)
        for d in range(1, n_pb):
            c_total = c_total + c_got[d - 1, rows].astype(F32)
        c_out[rows] = c_total.astype(BF16)
    for copy in copies:
        copy.wait_send()


def scatter(qg, cg):
    n_col, rows, width = qg.shape
    n_pb, crows, _ = cg.shape
    vmem = pl.BlockSpec(memory_space=pltpu.VMEM)
    block = (rows, width)
    dma = pltpu.SemaphoreType.DMA
    return pl.pallas_call(
        functools.partial(scatter_kernel, n_col, n_pb),
        out_shape=(jax.ShapeDtypeStruct(block, BF16), jax.ShapeDtypeStruct((crows, width), BF16)),
        in_specs=[vmem, vmem],
        out_specs=(vmem, vmem),
        scratch_shapes=[
            pltpu.VMEM((n_col, *block), BF16),
            pltpu.VMEM((n_col, *block), BF16),
            pltpu.VMEM((n_col, *block), BF16),
            pltpu.VMEM((n_col, *block), BF16),
            pltpu.VMEM((max(n_pb - 1, 1), crows, width), BF16),
        ]
        + [dma((n_col,))] * 6
        + [dma((n_pb,))] * 2,
        compiler_params=pltpu.CompilerParams(
            collective_id=2, has_side_effects=True, vmem_limit_bytes=60 * 2**20
        ),
        name="scatter",
    )(qg, cg)


def local(queries, candidates, grades, query_weights):
    n_col, n_pb = lax.axis_size("col"), lax.axis_size("pb")
    width = queries.shape[1]
    rows = queries.shape[0]
    scaling = 1.0 / math.sqrt(width)
    q_all, c_all, expo, stats = front(queries, candidates, grades, n_col, n_pb, scaling)
    c_block = c_all.reshape(-1, width)
    merged = merge(stats, grades.shape[1] * n_col)
    losses = merged[:, 2 * GRADES].reshape(-1)
    weights = query_weights.reshape(n_col, 1, rows)
    qg, cg = slope(expo, grades, q_all, c_block, stats, merged, weights, scaling)
    query_grad, cand_grad = scatter(qg, cg.reshape(n_pb, -1, width))
    return (losses, query_grad, cand_grad)


def solution(mesh):
    in_specs = (P(("pb", "col"), None), P(("col", "pb"), None), P("pb", "col"), P("pb"))
    out_specs = (P("pb"), P(("pb", "col"), None), P(("col", "pb"), None))
    return jax.shard_map(local, mesh=mesh, in_specs=in_specs, out_specs=out_specs, check_vma=False)
```

```python
import functools
import math

import jax
import jax.numpy as jnp
from jax import lax
from jax.experimental import pallas as pl
from jax.experimental.pallas import tpu as pltpu
from jax.sharding import PartitionSpec as P

GRADES = 5
STATS = 16
LOWEST = -1e30
MESH = pl.DeviceIdType.MESH
F32 = jnp.float32
BF16 = jnp.bfloat16


def dev(p, i):
    return {"pb": p, "col": i}


class Place:
    def __init__(self, n_col, n_pb):
        self.n_col, self.n_pb = n_col, n_pb
        self.cores = 2 if n_col % 2 == 0 else 1
        rest = n_col // self.cores
        self.mids = 2 if rest % 2 == 0 else 1
        self.outs = rest // self.mids
        self.me = lax.axis_index("col")
        self.p = lax.axis_index("pb")
        self.core = lax.rem(self.me, self.cores)
        chip = self.me // self.cores
        self.mid = lax.rem(chip, self.mids)
        self.out = chip // self.mids

    def index(self, do, dm, dc):
        o = lax.rem(self.out + do, self.outs)
        m = lax.rem(self.mid + dm, self.mids)
        c = lax.rem(self.core + dc, self.cores)
        return (o * self.mids + m) * self.cores + c

    def peers(self):
        found = [dev(self.p, self.index(d, 0, 0)) for d in range(1, self.outs)]
        found += [dev(self.p, self.index(0, d, 0)) for d in range(1, self.mids)]
        found += [dev(self.p, self.index(0, 0, d)) for d in range(1, self.cores)]
        found += [dev(lax.rem(self.p + d, self.n_pb), self.me) for d in range(1, self.n_pb)]
        return found


def greet(peers):
    barrier = pltpu.get_barrier_semaphore()
    for peer in peers:
        pl.semaphore_signal(barrier, inc=1, device_id=peer, device_id_type=MESH)
    pl.semaphore_wait(barrier, len(peers))


def remote(src, dst, send, recv, device):
    return pltpu.make_async_remote_copy(
        src_ref=src, dst_ref=dst, send_sem=send, recv_sem=recv, device_id=device, device_id_type=MESH
    )


def score_tile(scaling, q, c, grades):
    rows = grades.shape[0]
    scores = lax.dot_general(q, c, (((1,), (1,)), ((), ())), preferred_element_type=F32) * scaling
    lane = lax.broadcasted_iota(jnp.int32, (rows, rows), 1)
    table = jnp.zeros((rows, rows), F32)
    picked = jnp.zeros(scores.shape, F32)
    for b in range(GRADES):
        member = grades == b
        highest = jnp.max(jnp.where(member, scores, LOWEST), axis=1, keepdims=True)
        picked = jnp.where(member, highest, picked)
        table = jnp.where(lane == b, highest, table)
    expo = jnp.exp(scores - picked)
    for b in range(GRADES):
        member = grades == b
        mass = jnp.sum(jnp.where(member, expo, 0.0), axis=1, keepdims=True)
        table = jnp.where(lane == GRADES + b, mass, table)
    assert scores.shape[1] < 4096
    rest = jnp.full((rows, 1), float(scores.shape[1]), F32)
    for b in range(0, GRADES - 1, 2):
        pair = jnp.where(grades == b, 1.0, jnp.where(grades == b + 1, 4096.0, 0.0))
        pair = jnp.sum(pair, axis=1, keepdims=True)
        high = jnp.floor(pair * (1.0 / 4096.0))
        low = pair - high * 4096.0
        table = jnp.where(lane == 2 * GRADES + b, low, table)
        table = jnp.where(lane == 2 * GRADES + b + 1, high, table)
        rest = rest - low - high
    table = jnp.where(lane == 3 * GRADES - 1, rest, table)
    total = jnp.sum(scores, axis=1, keepdims=True)
    table = jnp.where(lane == 3 * GRADES, total, table)
    return expo, table.T[:STATS]


def front_kernel(
    n_col, n_pb, scaling, q_ref, c_ref, g_hbm, q_all, c_all, e_hbm, s_all,
    g_all, e_all, q_send, q_recv, c_send, c_recv, own_sem, e_sem,
):
    at = Place(n_col, n_pb)
    rows, half = q_ref.shape[0], c_ref.shape[0]
    grades_in = pltpu.make_async_copy(g_hbm, g_all, own_sem.at[0])
    grades_in.start()
    own = [
        pltpu.make_async_copy(q_ref, q_all.at[at.me], own_sem.at[1]),
        pltpu.make_async_copy(c_ref, c_all.at[at.p], own_sem.at[2]),
    ]
    for copy in own:
        copy.start()
    greet(at.peers())
    c_copies = []
    for d in range(1, n_pb):
        other = lax.rem(at.p + d, n_pb)
        copy = remote(c_ref, c_all.at[at.p], c_send.at[d], c_recv.at[at.p], dev(other, at.me))
        copy.start()
        c_copies.append(copy)
    sends = []

    def push(src, block, device):
        copy = remote(src, q_all.at[block], q_send.at[len(sends)], q_recv.at[block], device)
        copy.start()
        sends.append(copy)

    def arrived(block):
        remote(q_ref, q_all.at[block], q_send.at[0], q_recv.at[block], dev(at.p, at.me)).wait_recv()

    def forward(do, dm):
        block = at.index(do, dm, 0)
        src = q_ref
        if do or dm:
            arrived(block)
            src = q_all.at[block]
        if dm == 0:
            if do == 0:
                for d in order[1:]:
                    push(src, block, dev(at.p, at.index(d, 0, 0)))
            for d in range(1, at.mids):
                push(src, block, dev(at.p, at.index(0, d, 0)))
        for d in range(1, at.cores):
            push(src, block, dev(at.p, at.index(0, 0, d)))

    def task(block, part):
        span = pl.ds(pl.multiple_of(block * rows, rows), rows)
        columns = pl.ds(pl.multiple_of(part * half, half), half)
        expo, stats = score_tile(scaling, q_all[block], c_all[part], g_all[span, columns])
        e_all[block, part] = expo
        s_all[block, part] = stats
        pltpu.make_async_copy(
            e_all.at[block, part], e_hbm.at[block, part], e_sem.at[block, part]
        ).start()

    order = [0] + sorted(range(1, at.outs), key=lambda d: min(d, at.outs - d))
    last = order[-1]

    def group(pairs):
        first = pairs[0]
        step = [b - a for a, b in zip(first, pairs[-1])]

        def body(j, carry):
            which = j // at.cores
            dc = lax.rem(j, at.cores)
            block = at.index(first[0] + which * step[0], first[1] + which * step[1], dc)

            @pl.when(dc > 0)
            def _():
                arrived(block)

            task(block, at.p)
            return carry

        lax.fori_loop(0, len(pairs) * at.cores, body, 0)

    for k in range(at.outs):
        pairs = [(order[k], 0)]
        if k > 0 and at.mids > 1:
            pairs.append((order[k - 1], 1))
        for pair in pairs:
            forward(*pair)
        if k == 0:
            for copy in own:
                copy.wait()
            grades_in.wait()
        group(pairs)

    def later(first, count):
        for d in range(1, n_pb):
            part = lax.rem(at.p + d, n_pb)

            def body(j, carry):
                do = last + 1 + j // (at.mids * at.cores)
                dm = lax.rem(j // at.cores, at.mids)
                task(at.index(do, dm, lax.rem(j, at.cores)), part)
                return carry

            if first == 0:
                remote(
                    c_ref, c_all.at[part], c_send.at[0], c_recv.at[part], dev(at.p, at.me)
                ).wait_recv()
            lax.fori_loop(first, first + count, body, 0)

    tail = at.cores if at.mids > 1 else 0
    if tail:
        forward(last, 1)
    later(0, n_col - tail)
    if tail:
        group([(last, 1)])
        later(n_col - tail, tail)

    def drain(j, carry):
        for part in range(n_pb):
            pltpu.make_async_copy(e_all.at[j, part], e_hbm.at[j, part], e_sem.at[j, part]).wait()
        return carry

    lax.fori_loop(0, n_col, drain, 0)
    for copy in sends + c_copies:
        copy.wait_send()


def front(q, c, grades, n_col, n_pb, scaling):
    vmem = pl.BlockSpec(memory_space=pltpu.VMEM)
    hbm = pl.BlockSpec(memory_space=pl.ANY)
    rows, half = q.shape[0], c.shape[0]
    e_shape = (n_col, n_pb, rows, half)
    dma = pltpu.SemaphoreType.DMA
    return pl.pallas_call(
        functools.partial(front_kernel, n_col, n_pb, scaling),
        out_shape=(
            jax.ShapeDtypeStruct((n_col, *q.shape), q.dtype),
            jax.ShapeDtypeStruct((n_pb, *c.shape), c.dtype),
            jax.ShapeDtypeStruct(e_shape, F32),
            jax.ShapeDtypeStruct((n_col, n_pb, STATS, rows), F32),
        ),
        in_specs=[vmem, vmem, hbm],
        out_specs=(vmem, vmem, hbm, vmem),
        scratch_shapes=[
            pltpu.VMEM(grades.shape, jnp.int32),
            pltpu.VMEM(e_shape, F32),
            dma((2 * n_col,)),
            dma((n_col,)),
            dma((n_pb,)),
            dma((n_pb,)),
            dma((3,)),
            dma((n_col, n_pb)),
        ],
        compiler_params=pltpu.CompilerParams(
            collective_id=0, has_side_effects=True, vmem_limit_bytes=56 * 2**20
        ),
        name="front",
    )(q, c, grades)


def merge_kernel(n_col, columns, parts_ref, all_ref, s_ref, got, mine, send, recv, send2, recv2):
    me = lax.axis_index("col")
    p = lax.axis_index("pb")
    others = [lax.rem(me + d, n_col) for d in range(1, n_col)]
    greet([dev(p, o) for o in others])
    G = GRADES
    for k in range(n_col):
        parts = [parts_ref[k, h] for h in range(parts_ref.shape[1])]
        top = parts[0][:G]
        for part in parts[1:]:
            top = jnp.maximum(top, part[:G])
        mass = sum(part[G : 2 * G] * jnp.exp(part[:G] - top) for part in parts)
        s_ref[k] = jnp.concatenate([top, mass, sum(part[2 * G :] for part in parts)], axis=0)
    copies = []
    for d, o in enumerate(others):
        copy = remote(s_ref.at[o], got.at[me], send.at[d], recv.at[me], dev(p, o))
        copy.start()
        copies.append(copy)
    got[me] = s_ref[me]
    for o in others:
        remote(s_ref.at[o], got.at[o], send.at[0], recv.at[o], dev(p, o)).wait_recv()
    maxima = got[0][:G]
    for k in range(1, n_col):
        maxima = jnp.maximum(maxima, got[k][:G])
    masses = jnp.zeros_like(maxima)
    rest = jnp.zeros((STATS - 2 * G, maxima.shape[1]), F32)
    for k in range(n_col):
        block = got[k]
        masses = masses + block[G : 2 * G] * jnp.exp(block[:G] - maxima)
        rest = rest + block[2 * G :]
    mx = [maxima[b : b + 1] for b in range(G)]
    ms = [masses[b : b + 1] for b in range(G)]
    ct = [rest[b : b + 1] for b in range(G)]
    total = rest[G : G + 1]
    levels = []
    running = mx[0]
    seen = ct[0] * 0.0
    for b in range(G):
        running = jnp.maximum(running, mx[b])
        seen = seen + ct[b]
        summed = ms[0] * jnp.exp(mx[0] - running)
        for h in range(1, b + 1):
            summed = summed + ms[h] * jnp.exp(mx[h] - running)
        present = seen > 0.0
        levels.append(jnp.where(present, running + jnp.log(jnp.where(present, summed, 1.0)), running))
    weighted = ct[0] * levels[0]
    for b in range(1, G):
        weighted = weighted + ct[b] * levels[b]
    loss = (weighted - total) / columns
    factors = []
    for h in range(G):
        f = ct[h] * jnp.exp(mx[h] - levels[h])
        for b in range(h + 1, G):
            f = f + ct[b] * jnp.exp(mx[h] - levels[b])
        factors.append(f)
    pad = jnp.zeros((STATS - 2 * G - 1, loss.shape[1]), F32)
    mine[...] = jnp.concatenate(mx + factors + [loss, pad], axis=0)
    more = []
    for d, o in enumerate(others):
        copy = remote(mine, all_ref.at[me], send2.at[d], recv2.at[me], dev(p, o))
        copy.start()
        more.append(copy)
    all_ref[me] = mine[...]
    for o in others:
        remote(mine, all_ref.at[o], send2.at[0], recv2.at[o], dev(p, o)).wait_recv()
    for copy in copies + more:
        copy.wait_send()


def merge(stats, columns):
    n_col, _, _, rows = stats.shape
    shape = (n_col, STATS, rows)
    vmem = pl.BlockSpec(memory_space=pltpu.VMEM)
    return pl.pallas_call(
        functools.partial(merge_kernel, n_col, columns),
        out_shape=jax.ShapeDtypeStruct(shape, F32),
        in_specs=[vmem],
        out_specs=vmem,
        scratch_shapes=[
            pltpu.VMEM(shape, F32),
            pltpu.VMEM(shape, F32),
            pltpu.VMEM((STATS, rows), F32),
            pltpu.SemaphoreType.DMA((n_col,)),
            pltpu.SemaphoreType.DMA((n_col,)),
            pltpu.SemaphoreType.DMA((n_col,)),
            pltpu.SemaphoreType.DMA((n_col,)),
        ],
        compiler_params=pltpu.CompilerParams(collective_id=1, has_side_effects=True),
        name="merge",
    )(stats)


def slope_kernel(scaling, per, e_ref, g_ref, q_ref, c_ref, s_ref, f_ref, w_ref, qg_ref, cg_ref, acc):
    step = pl.program_id(0)
    G = GRADES
    rows = s_ref.shape[3]
    pieces = []
    n_pb = s_ref.shape[1]
    half = e_ref.shape[3]
    for k in range(per):
        merged, weight = f_ref[k], w_ref[k]
        factor = weight * merged[G : 2 * G]
        scaled = [factor * jnp.exp(s_ref[k, h, :G] - merged[:G]) for h in range(n_pb)]
        pad = jnp.zeros((rows - n_pb * G - 1, rows), F32)
        table = jnp.concatenate(scaled + [weight, pad], axis=0).T
        sections = []
        for h in range(n_pb):
            grades = g_ref[k * rows : (k + 1) * rows, h * half : (h + 1) * half]
            picked = jnp.broadcast_to(table[:, h * G : h * G + 1], grades.shape)
            for b in range(1, G):
                picked = jnp.where(grades == b, table[:, h * G + b : h * G + b + 1], picked)
            sections.append(picked * e_ref[k, h] - table[:, n_pb * G : n_pb * G + 1])
        slopes = jnp.concatenate(sections, axis=1)
        pieces.append(slopes.astype(BF16))
    slopes = jnp.concatenate(pieces, axis=0)
    part = jnp.dot(slopes, c_ref[...], preferred_element_type=F32) * scaling
    qg_ref[...] = part.astype(BF16).reshape(qg_ref.shape)
    term = lax.dot_general(
        slopes,
        q_ref[...].reshape(per * rows, -1),
        (((0,), (0,)), ((), ())),
        preferred_element_type=F32,
    )

    @pl.when(step == 0)
    def _():
        acc[...] = term

    @pl.when(step > 0)
    def _():
        acc[...] += term

    @pl.when(step == pl.num_programs(0) - 1)
    def _():
        cg_ref[...] = (acc[...] * scaling).astype(BF16)


def slope(expo, grades, q_all, c_block, stats, merged, weights, scaling):
    n, rows, width = q_all.shape
    cols = c_block.shape[0]
    per = 2 if n % 2 == 0 else 1
    block3 = lambda a, b: pl.BlockSpec((per, a, b), lambda i: (i, 0, 0))
    block4 = lambda a, b, c: pl.BlockSpec((per, a, b, c), lambda i: (i, 0, 0, 0))
    return pl.pallas_call(
        functools.partial(slope_kernel, scaling, per),
        grid=(n // per,),
        out_shape=(
            jax.ShapeDtypeStruct((n, rows, width), BF16),
            jax.ShapeDtypeStruct((cols, width), BF16),
        ),
        in_specs=[
            block4(*expo.shape[1:]),
            pl.BlockSpec((per * rows, cols), lambda i: (i, 0)),
            block3(rows, width),
            pl.BlockSpec((cols, width), lambda i: (0, 0)),
            block4(*stats.shape[1:]),
            block3(STATS, rows),
            block3(1, rows),
        ],
        out_specs=(block3(rows, width), pl.BlockSpec((cols, width), lambda i: (0, 0))),
        scratch_shapes=[pltpu.VMEM((cols, width), F32)],
        compiler_params=pltpu.CompilerParams(vmem_limit_bytes=48 * 2**20),
        name="slope",
    )(expo, grades, q_all, c_block, stats, merged, weights)


def scatter_kernel(
    n_col, n_pb, qg, cg, q_out, c_out,
    core_got, acc, mid_got, out_got, c_got,
    core_send, core_recv, mid_send, mid_recv, out_send, out_recv, c_send, c_recv,
):
    at = Place(n_col, n_pb)
    greet(at.peers())
    copies = []

    def push(*args):
        copy = remote(*args)
        copy.start()
        copies.append(copy)

    for d in range(1, n_pb):
        other = lax.rem(at.p + d, n_pb)
        push(cg.at[other], c_got.at[d - 1], c_send.at[d], c_recv.at[d - 1], dev(other, at.me))
    order = sorted(range(1, at.outs), key=lambda d: min(d, at.outs - d)) + [0]
    far = [(do, dm) for do in order for dm in range(1, at.mids)] + [(do, 0) for do in order]
    slot = {pair: k for k, pair in enumerate(far)}
    for do, dm in far:
        k = slot[do, dm]
        if at.cores > 1:
            push(
                qg.at[at.index(do, dm, 1)], core_got.at[k], core_send.at[k], core_recv.at[k],
                dev(at.p, at.index(0, 0, 1)),
            )

    def core_sum(do, dm):
        k = slot[do, dm]
        own = qg[at.index(do, dm, 0)].astype(F32)
        if at.cores > 1:
            remote(core_got.at[k], core_got.at[k], core_send.at[k], core_recv.at[k], dev(at.p, at.me)).wait_recv()
            own = own + core_got[k].astype(F32)
        return own

    for do in order:
        for dm in range(1, at.mids):
            k = slot[do, dm]
            acc[k] = core_sum(do, dm).astype(BF16)
            push(acc.at[k], mid_got.at[k], mid_send.at[k], mid_recv.at[k], dev(at.p, at.index(0, dm, 0)))
    for do in order:
        k = slot[do, 0]
        acc[k] = core_sum(do, 0).astype(BF16)
    for do in order:
        k = slot[do, 0]
        total = acc[k].astype(F32)
        for dm in range(1, at.mids):
            j = slot[do, dm]
            remote(acc.at[j], mid_got.at[j], mid_send.at[j], mid_recv.at[j], dev(at.p, at.me)).wait_recv()
            total = total + mid_got[j].astype(F32)
        if do:
            acc[k] = total.astype(BF16)
            push(acc.at[k], out_got.at[do - 1], out_send.at[do - 1], out_recv.at[do - 1], dev(at.p, at.index(do, 0, 0)))
    for d in range(1, at.outs):
        remote(acc.at[0], out_got.at[d - 1], out_send.at[d - 1], out_recv.at[d - 1], dev(at.p, at.me)).wait_recv()
        total = total + out_got[d - 1].astype(F32)
    q_out[...] = total.astype(BF16)
    for d in range(1, n_pb):
        remote(cg.at[0], c_got.at[d - 1], c_send.at[d], c_recv.at[d - 1], dev(at.p, at.me)).wait_recv()
    half = 128
    for r in range(0, c_out.shape[0], half):
        rows = pl.ds(r, half)
        c_total = cg[at.p, rows].astype(F32)
        for d in range(1, n_pb):
            c_total = c_total + c_got[d - 1, rows].astype(F32)
        c_out[rows] = c_total.astype(BF16)
    for copy in copies:
        copy.wait_send()


def scatter(qg, cg):
    n_col, rows, width = qg.shape
    n_pb, crows, _ = cg.shape
    vmem = pl.BlockSpec(memory_space=pltpu.VMEM)
    block = (rows, width)
    dma = pltpu.SemaphoreType.DMA
    return pl.pallas_call(
        functools.partial(scatter_kernel, n_col, n_pb),
        out_shape=(jax.ShapeDtypeStruct(block, BF16), jax.ShapeDtypeStruct((crows, width), BF16)),
        in_specs=[vmem, vmem],
        out_specs=(vmem, vmem),
        scratch_shapes=[
            pltpu.VMEM((n_col, *block), BF16),
            pltpu.VMEM((n_col, *block), BF16),
            pltpu.VMEM((n_col, *block), BF16),
            pltpu.VMEM((n_col, *block), BF16),
            pltpu.VMEM((max(n_pb - 1, 1), crows, width), BF16),
        ]
        + [dma((n_col,))] * 6
        + [dma((n_pb,))] * 2,
        compiler_params=pltpu.CompilerParams(
            collective_id=2, has_side_effects=True, vmem_limit_bytes=60 * 2**20
        ),
        name="scatter",
    )(qg, cg)


def local(queries, candidates, grades, query_weights):
    n_col, n_pb = lax.axis_size("col"), lax.axis_size("pb")
    width = queries.shape[1]
    rows = queries.shape[0]
    scaling = 1.0 / math.sqrt(width)
    q_all, c_all, expo, stats = front(queries, candidates, grades, n_col, n_pb, scaling)
    c_block = c_all.reshape(-1, width)
    merged = merge(stats, grades.shape[1] * n_col)
    losses = merged[:, 2 * GRADES].reshape(-1)
    weights = query_weights.reshape(n_col, 1, rows)
    qg, cg = slope(expo, grades, q_all, c_block, stats, merged, weights, scaling)
    query_grad, cand_grad = scatter(qg, cg.reshape(n_pb, -1, width))
    return (losses, query_grad, cand_grad)


def solution(mesh):
    in_specs = (P(("pb", "col"), None), P(("col", "pb"), None), P("pb", "col"), P("pb"))
    out_specs = (P("pb"), P(("pb", "col"), None), P(("col", "pb"), None))
    return jax.shard_map(local, mesh=mesh, in_specs=in_specs, out_specs=out_specs, check_vma=False)
```
